32 devices in a mesh: dp: 8 (over z, x), mp: 4 (over y, core).
Axes of the slice: x: 2, y: 2, z: 4, core: 2. Of those that a mesh axis runs over, the one named last changes fastest.
Arguments:
- query_rows: bfloat16 [2048, 2048], P('dp', 'mp'), may hold values from -6 to 6
- key_rows: bfloat16 [2048, 512], P('dp', 'mp'), may hold values from -6 to 6
- value_matrix: bfloat16 [2048, 512], P('dp', 'mp'), may hold values from -6 to 6
- out_weight: bfloat16 [2048, 5120], P('mp', 'dp'), may hold values from -0.125 to 0.125
- out_grad: bfloat16 [2048, 5120], P('dp', 'mp'), may hold values from -6 to 6
- doc_lengths: int32 [8, 8], P('dp'), may hold values from 1 to 249, as said below
Outputs:
- layer_out: bfloat16 [2048, 5120], P('dp', 'mp')
- query_grad: bfloat16 [2048, 2048], P('dp', 'mp')
- key_grad: bfloat16 [2048, 512], P('dp', 'mp')
- value_grad: bfloat16 [2048, 512], P('dp', 'mp')
- weight_grad: float32 [2048, 5120], P('mp', 'dp')
The draws below stay inside these ranges and needn't reach their ends.
Inputs may be any that keep to these rules, and one draw needn't show every extreme that they name: `doc_lengths`: each row holds 8 lengths of 1 or more that sum to 256.
All inputs are finite; a program needn't handle non-finite values.
Results may differ from the reference program's by a relative error of at most 0.014.
Values may be sent and summed in bfloat16 or wider, within the bound.
A program may use at most 64 MiB of HBM per device.

```python
import jax
import jax.numpy as jnp
from jax import lax

D = 5120
HQ = 16
KEY_VALUE_HEADS = 4
HEAD_WIDTH = 128
SEQ_DEV = 8
TOK_DEV = 256
TOKEN_TOTAL = 2048
N_DP = 8
N_MP = 4


def drawn_pair(key):
    base = jax.random.fold_in(key, 4021)
    query_key, key_random_seed = jax.random.split(base, 2)
    queries = jax.random.truncated_normal(query_key, -6.0, 6.0, (TOKEN_TOTAL, HQ * HEAD_WIDTH), jnp.float32)
    sampled_keys = jax.random.truncated_normal(key_random_seed, -6.0, 6.0, (TOKEN_TOTAL, KEY_VALUE_HEADS * HEAD_WIDTH), jnp.float32)
    return (queries, sampled_keys)


def draw_query_rows(key, part):
    return drawn_pair(key)[0].astype(jnp.bfloat16)


def draw_key_rows(key, part):
    return drawn_pair(key)[1].astype(jnp.bfloat16)


def draw_doc_lengths(key, part):
    base = jax.random.fold_in(key, 977)
    random_key, shift_key = jax.random.split(base)
    positions = jnp.arange(1, TOK_DEV, dtype=jnp.int32)
    shifts = jax.random.randint(shift_key, (N_DP, 1), 0, TOK_DEV, dtype=jnp.int32)
    device_rows = jnp.arange(N_DP, dtype=jnp.int32)[:, None]
    shifts = jnp.where(device_rows == 0, TOK_DEV - SEQ_DEV + 1, shifts)
    random_part = jax.random.randint(random_key, (N_DP, TOK_DEV - 1), 0, 4096, dtype=jnp.int32)
    scores = (random_part + 4096 * (positions[None, :] >= shifts).astype(jnp.int32)) * TOK_DEV + positions[None, :]
    picked = lax.top_k(scores, SEQ_DEV - 1)[1].astype(jnp.int32)
    cut_points = jnp.sort(picked + 1, axis=1)
    bounds = jnp.concatenate([jnp.zeros((N_DP, 1), jnp.int32), cut_points, jnp.full((N_DP, 1), TOK_DEV, jnp.int32)], axis=1)
    return jnp.diff(bounds, axis=1).astype(jnp.int32)


def raised(array, stream_key, source, target, parts, factor):
    def block_of(dim):
        return (jnp.arange(array.shape[dim]) // (array.shape[dim] // parts)).reshape((-1,) + (1,) * (array.ndim - 1 - dim))

    one_side = jax.random.permutation(stream_key, parts)[block_of(target)]
    other_side = (block_of(target) + parts // 2) % parts
    return jnp.where((block_of(source) == one_side) | (block_of(source) == other_side), factor * array, array)


def shard_levels(rng, extent, cuts, least, largest):
    gain = 1.0
    for axis_at, blocks in cuts:
        steps = jax.random.uniform(jax.random.fold_in(jax.random.fold_in(rng, 6), axis_at), (blocks,), jnp.float32, least / len(cuts), largest / len(cuts))
        gain = gain * jnp.repeat(jnp.exp(steps), extent[axis_at] // blocks).reshape((-1,) + (1,) * (len(extent) - 1 - axis_at))
    return gain


def normal_values(key, dims, spread, reach, shards=(), kind=jnp.bfloat16):
    drawn = spread * jax.random.normal(key, dims, jnp.float32)
    if shards:
        drawn = drawn * shard_levels(key, dims, shards, -0.22, 0.18)
    return jnp.clip(drawn, -reach, reach).astype(kind)


def gaussian_with(stream_key, extent, deviation, bound, cuts, heavy, kind=jnp.bfloat16):
    entries = deviation * jax.random.normal(stream_key, extent, jnp.float32)
    if cuts:
        entries = entries * shard_levels(stream_key, extent, cuts, -0.22, 0.18)
    return jnp.clip(raised(entries, jax.random.fold_in(stream_key, 3), *heavy), -bound, bound).astype(kind)


def setup_inputs(seed: int = 0) -> dict:
    streams_of = jax.random.split(jax.random.key(seed), 7)
    return {
        "query_rows": draw_query_rows(jax.random.fold_in(streams_of[6], 71), 0),
        "key_rows": draw_key_rows(jax.random.fold_in(streams_of[6], 71), 0),
        "value_matrix": normal_values(streams_of[2], (TOKEN_TOTAL, KEY_VALUE_HEADS * HEAD_WIDTH), 1.0, 6.0, ((0, 8), (1, 4))),
        "out_weight": normal_values(streams_of[3], (HQ * HEAD_WIDTH, D), (HQ * HEAD_WIDTH) ** -0.5, 0.125, ((0, 4), (1, 8))),
        "out_grad": gaussian_with(streams_of[4], (TOKEN_TOTAL, D), 1.0, 6.0, ((0, 8), (1, 4)), (0, 1, 8, 2.0)),
        "doc_lengths": draw_doc_lengths(jax.random.fold_in(streams_of[6], 71), 0),
    }


def local_segments(lengths, row_count):
    segment_ends = jnp.cumsum(lengths)
    positions = jnp.arange(row_count, dtype=jnp.int32)
    return jnp.sum((positions[:, None] >= segment_ends[None, :]).astype(jnp.int32), axis=1)


def split_heads(matrix):
    row_count = matrix.shape[0]
    return matrix.astype(jnp.float32).reshape(row_count, matrix.shape[1] // HEAD_WIDTH, HEAD_WIDTH).transpose(1, 0, 2)


def join_heads(tensor):
    return tensor.transpose(1, 0, 2).reshape(tensor.shape[1], tensor.shape[0] * HEAD_WIDTH)


def device_attention(queries_in, keys_in, values_in, upstream, segment):
    row_count = queries_in.shape[0]
    queries = split_heads(queries_in)
    kv_count = keys_in.shape[1] // HEAD_WIDTH
    group_size = queries.shape[0] // kv_count
    key_heads = jnp.repeat(split_heads(keys_in), group_size, axis=0)
    value_heads = jnp.repeat(split_heads(values_in), group_size, axis=0)
    upstreams = split_heads(upstream)
    softmax_scale = HEAD_WIDTH ** -0.5
    positions = jnp.arange(row_count, dtype=jnp.int32)
    allowed = (segment[:, None] == segment[None, :]) & (positions[:, None] >= positions[None, :])
    logits = jnp.einsum("hid,hjd->hij", queries, key_heads) * softmax_scale
    logits = jnp.where(allowed[None], logits, -jnp.inf)
    row_max = jnp.max(logits, axis=-1, keepdims=True)
    exp_terms = jnp.exp(logits - row_max)
    probability = exp_terms / jnp.sum(exp_terms, axis=-1, keepdims=True)
    weights = probability.astype(jnp.bfloat16).astype(jnp.float32)
    attended = jnp.einsum("hij,hjd->hid", weights, value_heads).astype(jnp.bfloat16)
    prob_grad = jnp.einsum("hid,hjd->hij", upstreams, value_heads)
    row_delta = jnp.sum(probability * prob_grad, axis=-1, keepdims=True)
    score_grad = (probability * (prob_grad - row_delta) * softmax_scale).astype(jnp.bfloat16).astype(jnp.float32)
    query_grad = jnp.einsum("hij,hjd->hid", score_grad, key_heads).astype(jnp.bfloat16)
    key_full = jnp.einsum("hij,hid->hjd", score_grad, queries)
    value_full = jnp.einsum("hij,hid->hjd", weights, upstreams)
    key_grad = key_full.reshape(kv_count, group_size, row_count, HEAD_WIDTH).sum(axis=1).astype(jnp.bfloat16)
    value_grad = value_full.reshape(kv_count, group_size, row_count, HEAD_WIDTH).sum(axis=1).astype(jnp.bfloat16)
    return join_heads(attended), join_heads(query_grad), join_heads(key_grad), join_heads(value_grad)


def reference(query_rows, key_rows, value_matrix, out_weight, out_grad, doc_lengths):
    attn_grad = jnp.dot(out_grad, out_weight.T, preferred_element_type=jnp.float32).astype(jnp.bfloat16)

    def per_device(pieces):
        queries_in, keys_in, values_in, upstream, lengths = pieces
        segment = local_segments(lengths, TOK_DEV)
        return device_attention(queries_in, keys_in, values_in, upstream, segment)

    stacked = (query_rows.reshape(N_DP, TOK_DEV, -1), key_rows.reshape(N_DP, TOK_DEV, -1),
               value_matrix.reshape(N_DP, TOK_DEV, -1), attn_grad.reshape(N_DP, TOK_DEV, -1), doc_lengths)
    attended, query_grad, key_grad, value_grad = lax.map(per_device, stacked)
    attended = attended.reshape(TOKEN_TOTAL, -1)
    query_grad = query_grad.reshape(TOKEN_TOTAL, -1)
    key_grad = key_grad.reshape(TOKEN_TOTAL, -1)
    value_grad = value_grad.reshape(TOKEN_TOTAL, -1)
    group_width = HQ * HEAD_WIDTH // N_MP
    total = jnp.zeros((TOKEN_TOTAL, D), jnp.float32)
    for group_index in range(N_MP):
        low_edge = group_index * group_width
        partial_sum = jnp.dot(attended[:, low_edge:low_edge + group_width], out_weight[low_edge:low_edge + group_width],
                              preferred_element_type=jnp.float32).astype(jnp.bfloat16)
        total = total + lax.optimization_barrier(partial_sum).astype(jnp.float32)
    layer_out = total.astype(jnp.bfloat16)
    weight_grad = jnp.dot(attended.T, out_grad, preferred_element_type=jnp.float32)
    return (layer_out, query_grad, key_grad, value_grad, weight_grad)
```

```python
import functools

import jax
import jax.numpy as jnp
from jax import lax
from jax.experimental import pallas as pl
from jax.experimental.pallas import tpu as pltpu
from jax.sharding import PartitionSpec as P

HEAD_WIDTH = 128
TILE = 128


def local_segments(lengths, row_count):
    segment_ends = jnp.cumsum(lengths)
    positions = jnp.arange(row_count, dtype=jnp.int32)
    return jnp.sum((positions[:, None] >= segment_ends[None, :]).astype(jnp.int32), axis=1)


def to_heads(matrix):
    return matrix.reshape(matrix.shape[0], matrix.shape[1] // HEAD_WIDTH, HEAD_WIDTH).transpose(
        1, 0, 2
    )


def from_heads(tensor):
    return tensor.transpose(1, 0, 2).reshape(tensor.shape[1], tensor.shape[0] * tensor.shape[2])


def attend(queries, key_rows, value_matrix, upstreams, segment):
    head_count, row_count, head_size = queries.shape
    tile_rows = min(TILE, row_count)
    block_count = row_count // tile_rows
    softmax_scale = HEAD_WIDTH ** (-0.5)
    offsets = jnp.arange(tile_rows, dtype=jnp.int32)
    empty_rows = jnp.zeros((tile_rows, head_size), jnp.float32)
    key_sums = [empty_rows] * block_count
    value_sums = [empty_rows] * block_count
    attended_blocks = []
    grad_blocks = []
    for block_index in range(block_count):
        row_start = block_index * tile_rows
        query_tile = queries[:, row_start : row_start + tile_rows]
        upstream_tile = upstreams[:, row_start : row_start + tile_rows]
        query_segment = segment[row_start : row_start + tile_rows]
        active = [
            segment[(column_index + 1) * tile_rows - 1] >= query_segment[0]
            for column_index in range(block_index + 1)
        ]
        score_tiles = []
        for column_index in range(block_index + 1):
            column_start = column_index * tile_rows
            key_tile = key_rows[column_start : column_start + tile_rows]
            key_segment = segment[column_start : column_start + tile_rows]
            allowed = (query_segment[:, None] == key_segment[None, :]) & (
                (row_start + offsets)[:, None] >= (column_start + offsets)[None, :]
            )

            def score_tile(query_tile=query_tile, key_tile=key_tile, allowed=allowed):
                logits = (
                    jnp.einsum(
                        "hid,jd->hij", query_tile, key_tile, preferred_element_type=jnp.float32
                    )
                    * softmax_scale
                )
                return jnp.where(allowed[None], logits, -jnp.inf)

            def masked_tile():
                return jnp.full((head_count, tile_rows, tile_rows), -jnp.inf, jnp.float32)

            score_tiles.append(lax.cond(active[column_index], score_tile, masked_tile))
        logits = jnp.concatenate(score_tiles, axis=-1)
        row_max = jnp.max(logits, axis=-1, keepdims=True)
        exp_terms = jnp.exp(logits - row_max)
        probability = exp_terms / jnp.sum(exp_terms, axis=-1, keepdims=True)
        weights = probability.astype(jnp.bfloat16)
        attended = jnp.zeros((head_count, tile_rows, head_size), jnp.float32)
        grad_tiles = []
        for column_index in range(block_index + 1):
            column_start = column_index * tile_rows
            value_tile = value_matrix[column_start : column_start + tile_rows]
            weight_tile = weights[:, :, column_start : column_start + tile_rows]

            def forward_tile(
                weight_tile=weight_tile, value_tile=value_tile, upstream_tile=upstream_tile
            ):
                return (
                    jnp.einsum(
                        "hij,jd->hid", weight_tile, value_tile, preferred_element_type=jnp.float32
                    ),
                    jnp.einsum(
                        "hid,jd->hij", upstream_tile, value_tile, preferred_element_type=jnp.float32
                    ),
                )

            def empty_pair():
                return (
                    jnp.zeros((head_count, tile_rows, head_size), jnp.float32),
                    jnp.zeros((head_count, tile_rows, tile_rows), jnp.float32),
                )

            contribution, prob_grad_tile = lax.cond(active[column_index], forward_tile, empty_pair)
            attended = attended + contribution
            grad_tiles.append(prob_grad_tile)
        prob_grad = jnp.concatenate(grad_tiles, axis=-1)
        row_delta = jnp.sum(probability * prob_grad, axis=-1, keepdims=True)
        score_grad = (probability * (prob_grad - row_delta) * softmax_scale).astype(jnp.bfloat16)
        query_sum = jnp.zeros((head_count, tile_rows, head_size), jnp.float32)
        for column_index in range(block_index + 1):
            column_start = column_index * tile_rows
            key_tile = key_rows[column_start : column_start + tile_rows]
            score_piece = score_grad[:, :, column_start : column_start + tile_rows]
            weight_tile = weights[:, :, column_start : column_start + tile_rows]

            def backward_tile(
                score_piece=score_piece,
                key_tile=key_tile,
                weight_tile=weight_tile,
                query_tile=query_tile,
                upstream_tile=upstream_tile,
            ):
                return (
                    jnp.einsum(
                        "hij,jd->hid", score_piece, key_tile, preferred_element_type=jnp.float32
                    ),
                    jnp.einsum(
                        "hij,hid->jd", score_piece, query_tile, preferred_element_type=jnp.float32
                    ),
                    jnp.einsum(
                        "hij,hid->jd",
                        weight_tile,
                        upstream_tile,
                        preferred_element_type=jnp.float32,
                    ),
                )

            def empty_triple():
                return (
                    jnp.zeros((head_count, tile_rows, head_size), jnp.float32),
                    empty_rows,
                    empty_rows,
                )

            query_part, key_part, value_part = lax.cond(
                active[column_index], backward_tile, empty_triple
            )
            query_sum = query_sum + query_part
            key_sums[column_index] = key_sums[column_index] + key_part
            value_sums[column_index] = value_sums[column_index] + value_part
        attended_blocks.append(attended.astype(jnp.bfloat16))
        grad_blocks.append(query_sum.astype(jnp.bfloat16))
    return (
        jnp.concatenate(attended_blocks, axis=1),
        jnp.concatenate(grad_blocks, axis=1),
        jnp.concatenate(key_sums, axis=0),
        jnp.concatenate(value_sums, axis=0),
    )


def grad_term(grad_full, attended_heads):
    attended_flat = from_heads(attended_heads)
    return lax.dot_general(
        grad_full, attended_flat, (((0,), (0,)), ((), ())), preferred_element_type=jnp.float32
    )


def per_device(query_rows, key_rows, value_matrix, out_weight, out_grad, doc_lengths):
    row_count = query_rows.shape[0]
    weight_full = lax.all_gather(out_weight, "dp", axis=1, tiled=True)
    grad_full = lax.all_gather(out_grad, "mp", axis=1, tiled=True)
    attn_grad = lax.dot_general(
        grad_full, weight_full, (((1,), (1,)), ((), ())), preferred_element_type=jnp.float32
    ).astype(jnp.bfloat16)
    segment = local_segments(doc_lengths[0], row_count)
    queries = to_heads(query_rows)
    upstreams = to_heads(attn_grad)
    attended, query_grad, key_sum, value_sum = attend(
        queries, key_rows, value_matrix, upstreams, segment
    )
    key_grad = key_sum.astype(jnp.bfloat16)
    value_grad = value_sum.astype(jnp.bfloat16)
    weight_part = lax.psum_scatter(
        grad_term(grad_full, attended), "dp", scatter_dimension=0, tiled=True
    )
    attended_flat = from_heads(attended)
    query_grad = from_heads(query_grad)
    partial_sum = jnp.dot(attended_flat, weight_full, preferred_element_type=jnp.float32).astype(
        jnp.bfloat16
    )
    layer_out = lax.psum_scatter(
        lax.optimization_barrier(partial_sum).astype(jnp.float32).astype(jnp.bfloat16),
        "mp",
        scatter_dimension=1,
        tiled=True,
    )
    return (layer_out, query_grad, key_grad, value_grad, weight_part.T)


def dot(a, b, dims):
    return lax.dot_general(a, b, (dims, ((), ())), preferred_element_type=jnp.float32)


NN = ((1,), (0,))
NT = ((1,), (1,))
TN = ((0,), (0,))


def allowed_pairs(lengths_ref, rows):
    row_at = lax.broadcasted_iota(jnp.int32, (rows, 1), 0)
    column_at = lax.broadcasted_iota(jnp.int32, (1, rows), 1)
    row_segment = jnp.zeros((rows, 1), jnp.int32)
    column_segment = jnp.zeros((1, rows), jnp.int32)
    end = jnp.int32(0)
    for index in range(lengths_ref.shape[1]):
        end = end + lengths_ref[0, index]
        row_segment = row_segment + jnp.where(row_at >= end, 1, 0)
        column_segment = column_segment + jnp.where(column_at >= end, 1, 0)
    return (row_segment == column_segment) & (row_at >= column_at)


def branch_kernel(
    n_dp,
    n_mp,
    lengths_ref,
    query_ref,
    key_ref,
    value_ref,
    weight_ref,
    grad_ref,
    layer_ref,
    query_grad_ref,
    key_grad_ref,
    value_grad_ref,
    weight_grad_ref,
    grads,
    heads_all,
    upstream_part,
    upstream_in,
    layer_part,
    layer_in,
    layer_sum,
    layer_done,
    probs,
    swap_send,
    grad_send,
    grad_recv,
    heads_send,
    heads_recv,
    up_send,
    up_recv,
    part_send,
    part_recv,
    done_send,
    done_recv,
):
    d = lax.axis_index("dp")
    m = lax.axis_index("mp")
    ratio = n_dp // n_mp
    rows = query_ref.shape[0]
    columns = weight_ref.shape[1]
    head_count = query_ref.shape[1] // HEAD_WIDTH
    group_size = query_ref.shape[1] // key_ref.shape[1]
    scale = HEAD_WIDTH ** (-0.5)
    home = lax.div(d, ratio)
    slot = lax.rem(d, ratio)

    def remote(source, target, send, recv, dp, mp):
        return pltpu.make_async_remote_copy(
            src_ref=source,
            dst_ref=target,
            send_sem=send,
            recv_sem=recv,
            device_id={"dp": dp, "mp": mp},
            device_id_type=pl.DeviceIdType.MESH,
        )

    def swap(j):
        return remote(
            grad_ref.at[:, pl.ds(j * columns, columns)],
            grads.at[d],
            swap_send.at[j],
            grad_recv.at[d],
            ratio * m + j,
            home,
        )

    def swap_here(j):
        return pltpu.make_async_copy(
            grad_ref.at[:, pl.ds(j * columns, columns)], grads.at[d], grad_recv.at[d]
        )

    def stays(j):
        return (home == m) & (slot == j)

    for j in range(ratio):
        @pl.when(jnp.logical_not(stays(j)))
        def _(j=j):
            swap(j).start()

        @pl.when(stays(j))
        def _(j=j):
            swap_here(j).start()

    allowed = allowed_pairs(lengths_ref, rows)
    for h in range(head_count):
        kv = h // group_size
        head = slice(h * HEAD_WIDTH, (h + 1) * HEAD_WIDTH)
        kv_head = slice(kv * HEAD_WIDTH, (kv + 1) * HEAD_WIDTH)
        logits = dot(query_ref[:, head], key_ref[:, kv_head], NT) * scale
        logits = jnp.where(allowed, logits, -jnp.inf)
        exp_terms = jnp.exp(logits - jnp.max(logits, axis=1, keepdims=True))
        probability = exp_terms / jnp.sum(exp_terms, axis=1, keepdims=True)
        probs[h] = probability
        heads_all[d, :, head] = dot(
            probability.astype(jnp.bfloat16), value_ref[:, kv_head], NN
        ).astype(jnp.bfloat16)

    def heads_copy(step):
        return remote(
            heads_all.at[d],
            heads_all.at[d],
            heads_send.at[step],
            heads_recv.at[d],
            lax.rem(d + step, n_dp),
            m,
        )

    def grad_copy(j, step):
        block = ratio * m + j
        return remote(
            grads.at[block],
            grads.at[block],
            grad_send.at[j, step],
            grad_recv.at[block],
            d,
            lax.rem(m + step, n_mp),
        )

    def grad_arrival(block):
        return remote(
            grads.at[block], grads.at[block], swap_send.at[0], grad_recv.at[block], d, m
        )

    def heads_arrival(block):
        return remote(
            heads_all.at[block], heads_all.at[block], swap_send.at[0], heads_recv.at[block], d, m
        )

    for step in range(1, n_dp):
        heads_copy(step).start()
    for j in range(ratio):
        grad_arrival(ratio * m + j).wait_recv()
        for step in range(1, n_mp):
            grad_copy(j, step).start()

    def up_copy(block):
        return remote(
            upstream_part.at[block],
            upstream_in.at[d],
            up_send.at[block],
            up_recv.at[d],
            block,
            m,
        )

    def up_step(index, carry):
        block = lax.rem(ratio * m + index, n_dp)

        @pl.when(index >= ratio)
        def _():
            grad_arrival(block).wait_recv()

        partial = dot(grads[block], weight_ref[...], NT).astype(jnp.bfloat16)

        @pl.when(block == d)
        def _():
            upstream_in[d] = partial

        @pl.when(block != d)
        def _():
            upstream_part[block] = partial
            up_copy(block).start()

        return carry

    lax.fori_loop(0, n_dp, up_step, 0)

    def part_copy(block):
        return remote(
            layer_part.at[block],
            layer_in.at[m, lax.rem(block, ratio)],
            part_send.at[block],
            part_recv.at[m, lax.rem(block, ratio)],
            d,
            lax.div(block, ratio),
        )

    def part_step(index, carry):
        block = lax.rem(d + index, n_dp)

        @pl.when(index >= 1)
        def _():
            heads_arrival(block).wait_recv()

        partial = dot(heads_all[block], weight_ref[...], NN).astype(jnp.bfloat16)

        @pl.when(lax.div(block, ratio) == m)
        def _():
            layer_in[m, lax.rem(block, ratio)] = partial

        @pl.when(lax.div(block, ratio) != m)
        def _():
            layer_part[block] = partial
            part_copy(block).start()

        return carry

    lax.fori_loop(0, n_dp, part_step, 0)

    weight_grad_ref[...] = jnp.zeros_like(weight_grad_ref)

    def weight_step(block, carry):
        weight_grad_ref[...] += dot(heads_all[block], grads[block], TN)
        return carry

    lax.fori_loop(0, n_dp, weight_step, 0)

    def part_arrival(source, j):
        return remote(
            layer_in.at[source, j],
            layer_in.at[source, j],
            swap_send.at[0],
            part_recv.at[source, j],
            d,
            m,
        )

    def done_copy(j):
        return remote(
            layer_sum.at[j],
            layer_done.at[slot],
            done_send.at[j],
            done_recv.at[slot],
            ratio * m + j,
            home,
        )

    for j in range(ratio):
        for step in range(1, n_mp):
            part_arrival(lax.rem(m + step, n_mp), j).wait_recv()
        total = layer_in[0, j].astype(jnp.float32)
        for source in range(1, n_mp):
            total = total + layer_in[source, j].astype(jnp.float32)
        layer_sum[j] = total.astype(jnp.bfloat16)

        @pl.when(jnp.logical_not(stays(j)))
        def _(j=j):
            done_copy(j).start()

        @pl.when(stays(j))
        def _(j=j):
            layer_done[j] = layer_sum[j]

    def up_arrival(block):
        return remote(
            upstream_in.at[block], upstream_in.at[block], swap_send.at[0], up_recv.at[block], d, m
        )

    for step in range(1, n_dp):
        up_arrival(lax.rem(d + step, n_dp)).wait_recv()
    for h in range(head_count):
        kv = h // group_size
        head = slice(h * HEAD_WIDTH, (h + 1) * HEAD_WIDTH)
        kv_head = slice(kv * HEAD_WIDTH, (kv + 1) * HEAD_WIDTH)
        upstream = upstream_in[0, :, head].astype(jnp.float32)
        for block in range(1, n_dp):
            upstream = upstream + upstream_in[block, :, head].astype(jnp.float32)
        upstream = upstream.astype(jnp.bfloat16)
        probability = probs[h]
        prob_grad = dot(upstream, value_ref[:, kv_head], NT)
        row_delta = jnp.sum(probability * prob_grad, axis=1, keepdims=True)
        score_grad = (probability * (prob_grad - row_delta) * scale).astype(jnp.bfloat16)
        query_grad_ref[:, head] = dot(score_grad, key_ref[:, kv_head], NN).astype(jnp.bfloat16)
        key_term = dot(score_grad, query_ref[:, head], TN)
        value_term = dot(probability.astype(jnp.bfloat16), upstream, TN)
        if h % group_size == 0:
            key_sum, value_sum = key_term, value_term
        else:
            key_sum, value_sum = key_sum + key_term, value_sum + value_term
        if h % group_size == group_size - 1:
            key_grad_ref[:, kv_head] = key_sum.astype(jnp.bfloat16)
            value_grad_ref[:, kv_head] = value_sum.astype(jnp.bfloat16)

    for j in range(ratio):
        @pl.when(jnp.logical_not(stays(j)))
        def _(j=j):
            remote(
                layer_done.at[j], layer_done.at[j], swap_send.at[0], done_recv.at[j], d, m
            ).wait_recv()

        layer_ref[:, j * columns : (j + 1) * columns] = layer_done[j]

    for j in range(ratio):
        @pl.when(jnp.logical_not(stays(j)))
        def _(j=j):
            swap(j).wait_send()
            done_copy(j).wait_send()

        for step in range(1, n_mp):
            grad_copy(j, step).wait_send()
    for step in range(1, n_dp):
        heads_copy(step).wait_send()

    def drain_step(block, carry):
        @pl.when(block != d)
        def _():
            up_copy(block).wait_send()

        @pl.when(lax.div(block, ratio) != m)
        def _():
            part_copy(block).wait_send()

        return carry

    lax.fori_loop(0, n_dp, drain_step, 0)


def fused(n_dp, n_mp, query_rows, key_rows, value_matrix, out_weight, out_grad, doc_lengths):
    rows, width = query_rows.shape
    columns = out_weight.shape[1]
    ratio = n_dp // n_mp
    vmem = pl.BlockSpec(memory_space=pltpu.VMEM)
    dma = pltpu.SemaphoreType.DMA
    return pl.pallas_call(
        functools.partial(branch_kernel, n_dp, n_mp),
        out_shape=(
            jax.ShapeDtypeStruct(out_grad.shape, jnp.bfloat16),
            jax.ShapeDtypeStruct(query_rows.shape, jnp.bfloat16),
            jax.ShapeDtypeStruct(key_rows.shape, jnp.bfloat16),
            jax.ShapeDtypeStruct(value_matrix.shape, jnp.bfloat16),
            jax.ShapeDtypeStruct(out_weight.shape, jnp.float32),
        ),
        in_specs=[pl.BlockSpec(memory_space=pltpu.SMEM)] + [vmem] * 5,
        out_specs=(vmem,) * 5,
        scratch_shapes=[
            pltpu.VMEM((n_dp, rows, columns), jnp.bfloat16),
            pltpu.VMEM((n_dp, rows, width), jnp.bfloat16),
            pltpu.VMEM((n_dp, rows, width), jnp.bfloat16),
            pltpu.VMEM((n_dp, rows, width), jnp.bfloat16),
            pltpu.VMEM((n_dp, rows, columns), jnp.bfloat16),
            pltpu.VMEM((n_mp, ratio, rows, columns), jnp.bfloat16),
            pltpu.VMEM((ratio, rows, columns), jnp.bfloat16),
            pltpu.VMEM((ratio, rows, columns), jnp.bfloat16),
            pltpu.VMEM((width // HEAD_WIDTH, rows, rows), jnp.float32),
            dma((ratio,)),
            dma((ratio, n_mp)),
            dma((n_dp,)),
            dma((n_dp,)),
            dma((n_dp,)),
            dma((n_dp,)),
            dma((n_dp,)),
            dma((n_dp,)),
            dma((n_mp, ratio)),
            dma((ratio,)),
            dma((ratio,)),
        ],
        compiler_params=pltpu.CompilerParams(
            has_side_effects=True, vmem_limit_bytes=56 * 1024 * 1024
        ),
    )(doc_lengths, query_rows, key_rows, value_matrix, out_weight, out_grad)


def body_of(n_dp, n_mp):
    def body(query_rows, key_rows, value_matrix, out_weight, out_grad, doc_lengths):
        arrays = (query_rows, key_rows, value_matrix, out_weight, out_grad, doc_lengths)
        columns = out_weight.shape[1]
        rows, width = query_rows.shape
        held = 2 * n_dp * rows * (4 * columns + 3 * width)
        if (
            columns % 128 == 0
            and rows % 128 == 0
            and n_dp % n_mp == 0
            and columns * (n_dp // n_mp) == out_grad.shape[1]
            and held < 24 * 1024 * 1024
        ):
            return fused(n_dp, n_mp, *arrays)
        return per_device(*arrays)

    return body


def solution(mesh):
    placed = (
        P("dp", "mp"),
        P("dp", "mp"),
        P("dp", "mp"),
        P("mp", "dp"),
        P("dp", "mp"),
        P("dp", None),
    )
    return jax.shard_map(
        body_of(mesh.shape["dp"], mesh.shape["mp"]),
        mesh=mesh,
        in_specs=placed,
        out_specs=(P("dp", "mp"), P("dp", "mp"), P("dp", "mp"), P("dp", "mp"), P("mp", "dp")),
        check_vma=False,
    )
```

```python
import functools

import jax
import jax.numpy as jnp
from jax import lax
from jax.experimental import pallas as pl
from jax.experimental.pallas import tpu as pltpu
from jax.sharding import PartitionSpec as P

HEAD_WIDTH = 128
TILE = 128


def local_segments(lengths, row_count):
    segment_ends = jnp.cumsum(lengths)
    positions = jnp.arange(row_count, dtype=jnp.int32)
    return jnp.sum((positions[:, None] >= segment_ends[None, :]).astype(jnp.int32), axis=1)


def to_heads(matrix):
    return matrix.reshape(matrix.shape[0], matrix.shape[1] // HEAD_WIDTH, HEAD_WIDTH).transpose(
        1, 0, 2
    )


def from_heads(tensor):
    return tensor.transpose(1, 0, 2).reshape(tensor.shape[1], tensor.shape[0] * tensor.shape[2])


def attend(queries, key_rows, value_matrix, upstreams, segment):
    head_count, row_count, head_size = queries.shape
    tile_rows = min(TILE, row_count)
    block_count = row_count // tile_rows
    softmax_scale = HEAD_WIDTH ** (-0.5)
    offsets = jnp.arange(tile_rows, dtype=jnp.int32)
    empty_rows = jnp.zeros((tile_rows, head_size), jnp.float32)
    key_sums = [empty_rows] * block_count
    value_sums = [empty_rows] * block_count
    attended_blocks = []
    grad_blocks = []
    for block_index in range(block_count):
        row_start = block_index * tile_rows
        query_tile = queries[:, row_start : row_start + tile_rows]
        upstream_tile = upstreams[:, row_start : row_start + tile_rows]
        query_segment = segment[row_start : row_start + tile_rows]
        active = [
            segment[(column_index + 1) * tile_rows - 1] >= query_segment[0]
            for column_index in range(block_index + 1)
        ]
        score_tiles = []
        for column_index in range(block_index + 1):
            column_start = column_index * tile_rows
            key_tile = key_rows[column_start : column_start + tile_rows]
            key_segment = segment[column_start : column_start + tile_rows]
            allowed = (query_segment[:, None] == key_segment[None, :]) & (
                (row_start + offsets)[:, None] >= (column_start + offsets)[None, :]
            )

            def score_tile(query_tile=query_tile, key_tile=key_tile, allowed=allowed):
                logits = (
                    jnp.einsum(
                        "hid,jd->hij", query_tile, key_tile, preferred_element_type=jnp.float32
                    )
                    * softmax_scale
                )
                return jnp.where(allowed[None], logits, -jnp.inf)

            def masked_tile():
                return jnp.full((head_count, tile_rows, tile_rows), -jnp.inf, jnp.float32)

            score_tiles.append(lax.cond(active[column_index], score_tile, masked_tile))
        logits = jnp.concatenate(score_tiles, axis=-1)
        row_max = jnp.max(logits, axis=-1, keepdims=True)
        exp_terms = jnp.exp(logits - row_max)
        probability = exp_terms / jnp.sum(exp_terms, axis=-1, keepdims=True)
        weights = probability.astype(jnp.bfloat16)
        attended = jnp.zeros((head_count, tile_rows, head_size), jnp.float32)
        grad_tiles = []
        for column_index in range(block_index + 1):
            column_start = column_index * tile_rows
            value_tile = value_matrix[column_start : column_start + tile_rows]
            weight_tile = weights[:, :, column_start : column_start + tile_rows]

            def forward_tile(
                weight_tile=weight_tile, value_tile=value_tile, upstream_tile=upstream_tile
            ):
                return (
                    jnp.einsum(
                        "hij,jd->hid", weight_tile, value_tile, preferred_element_type=jnp.float32
                    ),
                    jnp.einsum(
                        "hid,jd->hij", upstream_tile, value_tile, preferred_element_type=jnp.float32
                    ),
                )

            def empty_pair():
                return (
                    jnp.zeros((head_count, tile_rows, head_size), jnp.float32),
                    jnp.zeros((head_count, tile_rows, tile_rows), jnp.float32),
                )

            contribution, prob_grad_tile = lax.cond(active[column_index], forward_tile, empty_pair)
            attended = attended + contribution
            grad_tiles.append(prob_grad_tile)
        prob_grad = jnp.concatenate(grad_tiles, axis=-1)
        row_delta = jnp.sum(probability * prob_grad, axis=-1, keepdims=True)
        score_grad = (probability * (prob_grad - row_delta) * softmax_scale).astype(jnp.bfloat16)
        query_sum = jnp.zeros((head_count, tile_rows, head_size), jnp.float32)
        for column_index in range(block_index + 1):
            column_start = column_index * tile_rows
            key_tile = key_rows[column_start : column_start + tile_rows]
            score_piece = score_grad[:, :, column_start : column_start + tile_rows]
            weight_tile = weights[:, :, column_start : column_start + tile_rows]

            def backward_tile(
                score_piece=score_piece,
                key_tile=key_tile,
                weight_tile=weight_tile,
                query_tile=query_tile,
                upstream_tile=upstream_tile,
            ):
                return (
                    jnp.einsum(
                        "hij,jd->hid", score_piece, key_tile, preferred_element_type=jnp.float32
                    ),
                    jnp.einsum(
                        "hij,hid->jd", score_piece, query_tile, preferred_element_type=jnp.float32
                    ),
                    jnp.einsum(
                        "hij,hid->jd",
                        weight_tile,
                        upstream_tile,
                        preferred_element_type=jnp.float32,
                    ),
                )

            def empty_triple():
                return (
                    jnp.zeros((head_count, tile_rows, head_size), jnp.float32),
                    empty_rows,
                    empty_rows,
                )

            query_part, key_part, value_part = lax.cond(
                active[column_index], backward_tile, empty_triple
            )
            query_sum = query_sum + query_part
            key_sums[column_index] = key_sums[column_index] + key_part
            value_sums[column_index] = value_sums[column_index] + value_part
        attended_blocks.append(attended.astype(jnp.bfloat16))
        grad_blocks.append(query_sum.astype(jnp.bfloat16))
    return (
        jnp.concatenate(attended_blocks, axis=1),
        jnp.concatenate(grad_blocks, axis=1),
        jnp.concatenate(key_sums, axis=0),
        jnp.concatenate(value_sums, axis=0),
    )


def grad_term(grad_full, attended_heads):
    attended_flat = from_heads(attended_heads)
    return lax.dot_general(
        grad_full, attended_flat, (((0,), (0,)), ((), ())), preferred_element_type=jnp.float32
    )


def per_device(query_rows, key_rows, value_matrix, out_weight, out_grad, doc_lengths):
    row_count = query_rows.shape[0]
    weight_full = lax.all_gather(out_weight, "dp", axis=1, tiled=True)
    grad_full = lax.all_gather(out_grad, "mp", axis=1, tiled=True)
    attn_grad = lax.dot_general(
        grad_full, weight_full, (((1,), (1,)), ((), ())), preferred_element_type=jnp.float32
    ).astype(jnp.bfloat16)
    segment = local_segments(doc_lengths[0], row_count)
    queries = to_heads(query_rows)
    upstreams = to_heads(attn_grad)
    attended, query_grad, key_sum, value_sum = attend(
        queries, key_rows, value_matrix, upstreams, segment
    )
    key_grad = key_sum.astype(jnp.bfloat16)
    value_grad = value_sum.astype(jnp.bfloat16)
    weight_part = lax.psum_scatter(
        grad_term(grad_full, attended), "dp", scatter_dimension=0, tiled=True
    )
    attended_flat = from_heads(attended)
    query_grad = from_heads(query_grad)
    partial_sum = jnp.dot(attended_flat, weight_full, preferred_element_type=jnp.float32).astype(
        jnp.bfloat16
    )
    layer_out = lax.psum_scatter(
        lax.optimization_barrier(partial_sum).astype(jnp.float32).astype(jnp.bfloat16),
        "mp",
        scatter_dimension=1,
        tiled=True,
    )
    return (layer_out, query_grad, key_grad, value_grad, weight_part.T)


def dot(a, b, dims):
    return lax.dot_general(a, b, (dims, ((), ())), preferred_element_type=jnp.float32)


NN = ((1,), (0,))
NT = ((1,), (1,))
TN = ((0,), (0,))


def allowed_pairs(lengths_ref, rows):
    row_at = lax.broadcasted_iota(jnp.int32, (rows, 1), 0)
    column_at = lax.broadcasted_iota(jnp.int32, (1, rows), 1)
    row_segment = jnp.zeros((rows, 1), jnp.int32)
    column_segment = jnp.zeros((1, rows), jnp.int32)
    end = jnp.int32(0)
    for index in range(lengths_ref.shape[1]):
        end = end + lengths_ref[0, index]
        row_segment = row_segment + jnp.where(row_at >= end, 1, 0)
        column_segment = column_segment + jnp.where(column_at >= end, 1, 0)
    return (row_segment == column_segment) & (row_at >= column_at)


def branch_kernel(
    n_dp,
    n_mp,
    lengths_ref,
    query_ref,
    key_ref,
    value_ref,
    weight_ref,
    grad_ref,
    layer_ref,
    query_grad_ref,
    key_grad_ref,
    value_grad_ref,
    weight_grad_ref,
    grads,
    heads_all,
    upstream_part,
    twin_in,
    pair_sum,
    upstream_in,
    layer_part,
    layer_in,
    layer_sum,
    layer_done,
    probs,
    swap_send,
    grad_send,
    grad_recv,
    heads_send,
    heads_recv,
    up_send,
    twin_recv,
    pair_send,
    up_recv,
    part_send,
    part_recv,
    done_send,
    done_recv,
):
    d = lax.axis_index("dp")
    m = lax.axis_index("mp")
    ratio = n_dp // n_mp
    rows = query_ref.shape[0]
    columns = weight_ref.shape[1]
    head_count = query_ref.shape[1] // HEAD_WIDTH
    group_size = query_ref.shape[1] // key_ref.shape[1]
    scale = HEAD_WIDTH ** (-0.5)
    home = lax.div(d, ratio)
    slot = lax.rem(d, ratio)
    keeper = lax.rem(d, n_mp)
    line = n_dp // 2
    spot = lax.div(d, 2)
    side = lax.rem(d, 2)
    twin = 2 * spot + 1 - side
    sibling = 2 * lax.div(m, 2) + 1 - lax.rem(m, 2)

    def remote(source, target, send, recv, dp, mp):
        return pltpu.make_async_remote_copy(
            src_ref=source,
            dst_ref=target,
            send_sem=send,
            recv_sem=recv,
            device_id={"dp": dp, "mp": mp},
            device_id_type=pl.DeviceIdType.MESH,
        )

    def swap(j):
        return remote(
            grad_ref.at[:, pl.ds(j * columns, columns)],
            grads.at[d],
            swap_send.at[j],
            grad_recv.at[d],
            ratio * m + j,
            keeper,
        )

    def swap_here(j):
        return pltpu.make_async_copy(
            grad_ref.at[:, pl.ds(j * columns, columns)], grads.at[d], grad_recv.at[d]
        )

    def stays(j):
        return (keeper == m) & (d == ratio * m + j)

    def summed_here(j):
        return (home == m) & (d == m + n_mp * j)

    for j in range(ratio):
        @pl.when(jnp.logical_not(stays(j)))
        def _(j=j):
            swap(j).start()

        @pl.when(stays(j))
        def _(j=j):
            swap_here(j).start()

    allowed = allowed_pairs(lengths_ref, rows)
    for h in range(head_count):
        kv = h // group_size
        head = slice(h * HEAD_WIDTH, (h + 1) * HEAD_WIDTH)
        kv_head = slice(kv * HEAD_WIDTH, (kv + 1) * HEAD_WIDTH)
        logits = dot(query_ref[:, head], key_ref[:, kv_head], NT) * scale
        logits = jnp.where(allowed, logits, -jnp.inf)
        exp_terms = jnp.exp(logits - jnp.max(logits, axis=1, keepdims=True))
        probability = exp_terms / jnp.sum(exp_terms, axis=1, keepdims=True)
        probs[h] = probability
        heads_all[d, :, head] = dot(
            probability.astype(jnp.bfloat16), value_ref[:, kv_head], NN
        ).astype(jnp.bfloat16)

    def heads_copy(block, way):
        target = (d + 2, d - 2, twin)[way]
        return remote(
            heads_all.at[block],
            heads_all.at[block],
            heads_send.at[block, way],
            heads_recv.at[block],
            target,
            m,
        )

    def heads_pass(distance, started):
        def act(block, way):
            if started:
                heads_copy(block, way).start()
            else:
                heads_copy(block, way).wait_send()

        for way, sign in ((0, -1), (1, 1)):
            block = d + sign * 2 * distance
            origin = spot + sign * distance
            onward = spot - sign

            @pl.when((origin >= 0) & (origin < line))
            def _(block=block, way=way, onward=onward):
                if started and distance > 0:
                    heads_arrival(block).wait_recv()

                @pl.when((onward >= 0) & (onward < line))
                def _():
                    act(block, way)

                if distance > 0:
                    act(block, 2)
        if distance == 0:
            act(d, 2)

    def grad_copy(block, step, mp):
        return remote(
            grads.at[block],
            grads.at[block],
            grad_send.at[lax.div(block, n_mp), step],
            grad_recv.at[block],
            d,
            mp,
        )

    def own_grad(j):
        return [grad_copy(m + n_mp * j, 0, sibling)] + [
            grad_copy(m + n_mp * j, step, lax.rem(m + 2 * step, n_mp))
            for step in range(1, n_mp // 2)
        ]

    def across(j, step):
        return lax.rem(m + n_mp - 2 * step, n_mp) + n_mp * j

    def passed_grad(j, step):
        return grad_copy(across(j, step), n_mp // 2 - 1 + step, sibling)

    def grad_arrival(block):
        return remote(
            grads.at[block], grads.at[block], swap_send.at[0], grad_recv.at[block], d, m
        )

    def heads_arrival(block):
        return remote(
            heads_all.at[block], heads_all.at[block], swap_send.at[0], heads_recv.at[block], d, m
        )

    heads_pass(0, True)
    for j in range(ratio):
        grad_arrival(m + n_mp * j).wait_recv()
        for copy in own_grad(j):
            copy.start()

    def up_copy(block):
        return remote(
            upstream_part.at[block],
            twin_in.at[lax.div(block, 2)],
            up_send.at[block],
            twin_recv.at[lax.div(block, 2)],
            twin,
            m,
        )

    def up_block(block):
        upstream_part[block] = dot(grads[block], weight_ref[...], NT).astype(jnp.bfloat16)

        @pl.when(lax.rem(block, 2) != side)
        def _():
            up_copy(block).start()

    def own_step(index, carry):
        up_block(m + n_mp * index)
        return carry

    lax.fori_loop(0, ratio, own_step, 0)
    for step in range(1, n_mp // 2):
        for j in range(ratio):
            grad_arrival(across(j, step)).wait_recv()
            passed_grad(j, step).start()
    heads_pass(1, True)

    def near_step(index, carry):
        up_block(lax.rem(m + n_mp - 2 * (1 + lax.div(index, ratio)), n_mp) + n_mp * lax.rem(index, ratio))
        return carry

    lax.fori_loop(0, ratio * (n_mp // 2 - 1), near_step, 0)

    def far_step(index, carry):
        block = lax.rem(sibling + n_mp - 2 * lax.div(index, ratio), n_mp) + n_mp * lax.rem(index, ratio)
        grad_arrival(block).wait_recv()
        up_block(block)
        return carry

    lax.fori_loop(0, ratio, far_step, 0)
    for distance in range(2, line):
        heads_pass(distance, True)
    lax.fori_loop(ratio, ratio * (n_mp // 2), far_step, 0)

    def pair_copy(place):
        return remote(
            pair_sum.at[place],
            upstream_in.at[spot],
            pair_send.at[place],
            up_recv.at[spot],
            2 * place + side,
            m,
        )

    def pair_step(index, carry):
        place = lax.rem(spot + 1 + index, line)
        remote(
            twin_in.at[place], twin_in.at[place], swap_send.at[0], twin_recv.at[place], d, m
        ).wait_recv()
        total = (
            upstream_part[2 * place + side].astype(jnp.float32)
            + twin_in[place].astype(jnp.float32)
        ).astype(jnp.bfloat16)

        @pl.when(place == spot)
        def _():
            upstream_in[spot] = total

        @pl.when(place != spot)
        def _():
            pair_sum[place] = total
            pair_copy(place).start()

        return carry

    def part_copy(block):
        return remote(
            layer_part.at[block],
            layer_in.at[m, lax.div(block, n_mp)],
            part_send.at[block],
            part_recv.at[m, lax.div(block, n_mp)],
            d,
            lax.rem(block, n_mp),
        )

    def part_step(index, carry):
        block = lax.rem(lax.rem(d + 2 * index, n_dp) + lax.div(index, line) * (twin - d) + n_dp, n_dp)

        @pl.when(index >= line)
        def _():
            heads_arrival(block).wait_recv()

        partial = dot(heads_all[block], weight_ref[...], NN).astype(jnp.bfloat16)

        @pl.when(lax.rem(block, n_mp) == m)
        def _():
            layer_in[m, lax.div(block, n_mp)] = partial

        @pl.when(lax.rem(block, n_mp) != m)
        def _():
            layer_part[block] = partial
            part_copy(block).start()

        return carry

    lax.fori_loop(0, line, part_step, 0)
    lax.fori_loop(0, line, pair_step, 0)
    lax.fori_loop(line, n_dp, part_step, 0)

    weight_grad_ref[...] = jnp.zeros_like(weight_grad_ref)

    def weight_step(block, carry):
        weight_grad_ref[...] += dot(heads_all[block], grads[block], TN)
        return carry

    lax.fori_loop(0, n_dp, weight_step, 0)

    def part_arrival(source, j):
        return remote(
            layer_in.at[source, j],
            layer_in.at[source, j],
            swap_send.at[0],
            part_recv.at[source, j],
            d,
            m,
        )

    def done_copy(j):
        return remote(
            layer_sum.at[j],
            layer_done.at[slot],
            done_send.at[j],
            done_recv.at[slot],
            m + n_mp * j,
            home,
        )

    for j in range(ratio):
        for step in range(1, n_mp):
            part_arrival(lax.rem(m + step, n_mp), j).wait_recv()
        total = layer_in[0, j].astype(jnp.float32)
        for source in range(1, n_mp):
            total = total + layer_in[source, j].astype(jnp.float32)
        layer_sum[j] = total.astype(jnp.bfloat16)

        @pl.when(jnp.logical_not(summed_here(j)))
        def _(j=j):
            done_copy(j).start()

        @pl.when(summed_here(j))
        def _(j=j):
            layer_done[slot] = layer_sum[j]

    def up_arrival(block):
        return remote(
            upstream_in.at[block], upstream_in.at[block], swap_send.at[0], up_recv.at[block], d, m
        )

    for step in range(1, line):
        up_arrival(lax.rem(spot + step, line)).wait_recv()
    for h in range(head_count):
        kv = h // group_size
        head = slice(h * HEAD_WIDTH, (h + 1) * HEAD_WIDTH)
        kv_head = slice(kv * HEAD_WIDTH, (kv + 1) * HEAD_WIDTH)
        upstream = upstream_in[0, :, head].astype(jnp.float32)
        for block in range(1, line):
            upstream = upstream + upstream_in[block, :, head].astype(jnp.float32)
        upstream = upstream.astype(jnp.bfloat16)
        probability = probs[h]
        prob_grad = dot(upstream, value_ref[:, kv_head], NT)
        row_delta = jnp.sum(probability * prob_grad, axis=1, keepdims=True)
        score_grad = (probability * (prob_grad - row_delta) * scale).astype(jnp.bfloat16)
        query_grad_ref[:, head] = dot(score_grad, key_ref[:, kv_head], NN).astype(jnp.bfloat16)
        key_term = dot(score_grad, query_ref[:, head], TN)
        value_term = dot(probability.astype(jnp.bfloat16), upstream, TN)
        if h % group_size == 0:
            key_sum, value_sum = key_term, value_term
        else:
            key_sum, value_sum = key_sum + key_term, value_sum + value_term
        if h % group_size == group_size - 1:
            key_grad_ref[:, kv_head] = key_sum.astype(jnp.bfloat16)
            value_grad_ref[:, kv_head] = value_sum.astype(jnp.bfloat16)

    for j in range(ratio):
        @pl.when(jnp.logical_not(stays(j)))
        def _(j=j):
            remote(
                layer_done.at[j], layer_done.at[j], swap_send.at[0], done_recv.at[j], d, m
            ).wait_recv()

        layer_ref[:, j * columns : (j + 1) * columns] = layer_done[j]

    for j in range(ratio):
        @pl.when(jnp.logical_not(stays(j)))
        def _(j=j):
            swap(j).wait_send()

        @pl.when(jnp.logical_not(summed_here(j)))
        def _(j=j):
            done_copy(j).wait_send()

        for copy in own_grad(j):
            copy.wait_send()
        for step in range(1, n_mp // 2):
            passed_grad(j, step).wait_send()
    for distance in range(line):
        heads_pass(distance, False)
    for step in range(1, line):
        pair_copy(lax.rem(spot + step, line)).wait_send()

    def drain_step(block, carry):
        @pl.when(lax.rem(block, 2) != side)
        def _():
            up_copy(block).wait_send()

        @pl.when(lax.rem(block, n_mp) != m)
        def _():
            part_copy(block).wait_send()

        return carry

    lax.fori_loop(0, n_dp, drain_step, 0)


def fused(n_dp, n_mp, query_rows, key_rows, value_matrix, out_weight, out_grad, doc_lengths):
    rows, width = query_rows.shape
    columns = out_weight.shape[1]
    ratio = n_dp // n_mp
    vmem = pl.BlockSpec(memory_space=pltpu.VMEM)
    dma = pltpu.SemaphoreType.DMA
    return pl.pallas_call(
        functools.partial(branch_kernel, n_dp, n_mp),
        out_shape=(
            jax.ShapeDtypeStruct(out_grad.shape, jnp.bfloat16),
            jax.ShapeDtypeStruct(query_rows.shape, jnp.bfloat16),
            jax.ShapeDtypeStruct(key_rows.shape, jnp.bfloat16),
            jax.ShapeDtypeStruct(value_matrix.shape, jnp.bfloat16),
            jax.ShapeDtypeStruct(out_weight.shape, jnp.float32),
        ),
        in_specs=[pl.BlockSpec(memory_space=pltpu.SMEM)] + [vmem] * 5,
        out_specs=(vmem,) * 5,
        scratch_shapes=[
            pltpu.VMEM((n_dp, rows, columns), jnp.bfloat16),
            pltpu.VMEM((n_dp, rows, width), jnp.bfloat16),
            pltpu.VMEM((n_dp, rows, width), jnp.bfloat16),
            pltpu.VMEM((n_dp // 2, rows, width), jnp.bfloat16),
            pltpu.VMEM((n_dp // 2, rows, width), jnp.bfloat16),
            pltpu.VMEM((n_dp // 2, rows, width), jnp.bfloat16),
            pltpu.VMEM((n_dp, rows, columns), jnp.bfloat16),
            pltpu.VMEM((n_mp, ratio, rows, columns), jnp.bfloat16),
            pltpu.VMEM((ratio, rows, columns), jnp.bfloat16),
            pltpu.VMEM((ratio, rows, columns), jnp.bfloat16),
            pltpu.VMEM((width // HEAD_WIDTH, rows, rows), jnp.float32),
            dma((ratio,)),
            dma((ratio, n_mp)),
            dma((n_dp,)),
            dma((n_dp, 3)),
            dma((n_dp,)),
            dma((n_dp,)),
            dma((n_dp // 2,)),
            dma((n_dp // 2,)),
            dma((n_dp // 2,)),
            dma((n_dp,)),
            dma((n_mp, ratio)),
            dma((ratio,)),
            dma((ratio,)),
        ],
        compiler_params=pltpu.CompilerParams(
            has_side_effects=True, vmem_limit_bytes=56 * 1024 * 1024
        ),
    )(doc_lengths, query_rows, key_rows, value_matrix, out_weight, out_grad)


def body_of(n_dp, n_mp):
    def body(query_rows, key_rows, value_matrix, out_weight, out_grad, doc_lengths):
        arrays = (query_rows, key_rows, value_matrix, out_weight, out_grad, doc_lengths)
        columns = out_weight.shape[1]
        rows, width = query_rows.shape
        held = 2 * n_dp * rows * (4 * columns + 3 * width)
        if (
            columns % 128 == 0
            and rows % 128 == 0
            and n_dp % n_mp == 0
            and n_mp % 2 == 0
            and columns * (n_dp // n_mp) == out_grad.shape[1]
            and held < 24 * 1024 * 1024
        ):
            return fused(n_dp, n_mp, *arrays)
        return per_device(*arrays)

    return body


def solution(mesh):
    placed = (
        P("dp", "mp"),
        P("dp", "mp"),
        P("dp", "mp"),
        P("mp", "dp"),
        P("dp", "mp"),
        P("dp", None),
    )
    return jax.shard_map(
        body_of(mesh.shape["dp"], mesh.shape["mp"]),
        mesh=mesh,
        in_specs=placed,
        out_specs=(P("dp", "mp"), P("dp", "mp"), P("dp", "mp"), P("dp", "mp"), P("mp", "dp")),
        check_vma=False,
    )
```
